32 devices in a mesh: vec: 4 (over z), field: 4 (over x, core), rep: 2 (over y).
Axes of the slice: x: 2, y: 2, z: 4, core: 2. Of those that a mesh axis runs over, the one named last changes fastest.
Arguments:
- dosage: bfloat16 [96, 65536], P('vec', 'field'), may hold values from 0 to 2
Outputs:
- ccc: float32 [2, 96, 2, 24, 2, 96], P('rep', ('vec', 'field'))
The draws below stay inside these ranges and needn't reach their ends.
All inputs are finite; a program needn't handle non-finite values.
Results may differ from the reference program's by a relative error of at most 0.0003.
Values may be sent and summed in bfloat16 or wider, within the bound.
A program may use at most 64 MiB of HBM per device.

```python
import jax
import jax.numpy as jnp
from jax import lax

F = 65536
VB = 24
S = 2
V = 96
N_VEC = 4
N_REP = 2


def draw_dosage(key, part):
    freq_key, noise_key = jax.random.split(jax.random.fold_in(key, 11), 2)
    position = jnp.arange(F, dtype=jnp.float32) / F
    allele = (0.12 + 0.6 * position) * jax.random.uniform(freq_key, (F,), jnp.float32, 0.6, 1.4)
    dosage_value = 2.0 * allele[None, :] + 0.5 * jax.random.normal(noise_key, (V, F), jnp.float32)
    return jnp.clip(dosage_value, 0.0, 2.0).astype(jnp.bfloat16)


def setup_inputs(seed: int = 0) -> dict:
    key_list = jax.random.split(jax.random.key(seed), 2)
    dosage = draw_dosage(jax.random.fold_in(key_list[1], 71), 0)
    return {"dosage": dosage}


def contract_rows(first_rows, third_rows, partner_rows):
    field_width = first_rows.shape[1]
    block_width = min(2048, field_width)
    block_count = field_width // block_width

    def add_block(running, block_id):
        offset = block_id * block_width
        first_cut = lax.dynamic_slice_in_dim(first_rows, offset, block_width, 1)
        third_cut = lax.dynamic_slice_in_dim(third_rows, offset, block_width, 1)
        partner_cut = lax.dynamic_slice_in_dim(partner_rows, offset, block_width, 1)
        pair_rows = (first_cut[:, None, :] * third_cut[None, :, :]).reshape(-1, block_width)
        running = running + lax.dot_general(pair_rows.astype(jnp.float32), partner_cut.astype(jnp.float32), (((1,), (1,)), ((), ())), precision=lax.Precision.HIGHEST, preferred_element_type=jnp.float32)
        return running, None

    start_value = jnp.zeros((first_rows.shape[0] * third_rows.shape[0], partner_rows.shape[0]), jnp.float32)
    running, unused = lax.scan(add_block, start_value, jnp.arange(block_count, dtype=jnp.int32))
    return running


def reference(dosage):
    other_count = (2.0 - dosage.astype(jnp.float32)).astype(jnp.bfloat16)
    stacked = jnp.stack([other_count, dosage], axis=1)
    totals = jnp.sum(stacked.astype(jnp.float32), axis=2)
    gain_all = (1.0 - totals / (3.0 * F)).reshape(N_VEC, VB, 2)
    vector_rows = stacked.reshape(N_VEC, 2 * VB, F)
    planes = []
    for rep_plane in range(N_REP):
        def plane_block(block_id):
            third_id = (block_id - 1 - rep_plane) % N_VEC
            partner_ids = (block_id + 1 + jnp.arange(S, dtype=jnp.int32)) % N_VEC
            partner_rows = vector_rows[partner_ids].reshape(S * 2 * VB, F)
            tables = contract_rows(vector_rows[block_id], vector_rows[third_id], partner_rows)
            tables = tables.reshape(VB, 2, VB, 2, S * 2 * VB)
            gain_first = gain_all[block_id]
            gain_third = gain_all[third_id]
            gain_partner = gain_all[partner_ids].reshape(-1)
            return (4.5 / (8.0 * F)) * tables * gain_first[:, :, None, None, None] * gain_third[None, None, :, :, None] * gain_partner
        planes.append(lax.map(plane_block, jnp.arange(N_VEC, dtype=jnp.int32)))
    return jnp.stack(planes).reshape(N_REP, V, 2, VB, 2, S * 2 * VB)
```

```python
import functools

import jax
import jax.numpy as jnp
from jax import lax
from jax.experimental import pallas as pl
from jax.experimental.pallas import tpu as pltpu
from jax.sharding import PartitionSpec as P

MESH = pl.DeviceIdType.MESH
CHUNKS = 4
STEP = 512


def kernel(nv, nf, nr, fields, d_ref, o_ref, own, low, high, far, acc, outgoing, incoming,
           load_sem, ring_send, ring_recv, hop_send, hop_recv, table_send, table_recv):
    groups, _, half = own.shape
    vectors = groups * 8
    share = vectors // nf
    pair_rows = vectors * vectors
    plane_rows = pair_rows + vectors
    shared_far = far.shape[0] == 1
    width = half // CHUNKS
    members = nf * nr

    vec_at = lax.axis_index("vec")
    field_at = lax.axis_index("field")
    rep_at = lax.axis_index("rep")
    place = rep_at * nf + field_at
    above = {"vec": lax.rem(vec_at + 1, nv)}
    below = {"vec": lax.rem(vec_at + nv - 1, nv)}

    def member(offset):
        index = lax.rem(place + offset, members)
        return index, {"rep": index // nf, "field": lax.rem(index, nf)}

    load = pltpu.make_async_copy(
        d_ref.at[:, :, pl.ds(pl.multiple_of(rep_at * half, half), half)], own, load_sem
    )
    load.start()
    barrier = pltpu.get_barrier_semaphore()
    for target in (above, below):
        pl.semaphore_signal(barrier, inc=1, device_id=target, device_id_type=MESH)
    for offset in range(1, members):
        pl.semaphore_signal(barrier, inc=1, device_id=member(offset)[1], device_id_type=MESH)
    acc[...] = jnp.zeros_like(acc)
    load.wait()
    pl.semaphore_wait(barrier, members + 1)

    def own_copies(c):
        cut = pl.ds(c * width, width)
        return [
            pltpu.make_async_remote_copy(
                src_ref=own.at[:, :, cut], dst_ref=buffer.at[:, :, cut],
                send_sem=ring_send.at[way, c], recv_sem=ring_recv.at[way, c],
                device_id=target, device_id_type=MESH)
            for way, (buffer, target) in enumerate(((low, above), (high, below)))
        ]

    def hop_copies(c):
        copies = []
        for way, (buffer, target) in enumerate(((low, above), (high, below))):
            if shared_far:
                cut = pl.ds(c * width + way * (width // 2), width // 2)
                landing = far.at[0, :, :, cut]
            else:
                cut = pl.ds(c * width, width)
                landing = far.at[way, :, :, cut]
            copies.append(pltpu.make_async_remote_copy(
                src_ref=buffer.at[:, :, cut], dst_ref=landing,
                send_sem=hop_send.at[way, c], recv_sem=hop_recv.at[way, c],
                device_id=target, device_id_type=MESH))
        return copies

    def contract(c):
        def step(t, carry):
            cut = pl.ds(pl.multiple_of(c * width + t * STEP, STEP), STEP)

            def rows(block):
                return block.astype(jnp.float32).reshape(vectors, STEP)

            mine = rows(own[:, :, cut])
            thirds = [rows(low[:, :, cut]), rows(far[0, :, :, cut])]
            partners = [rows(high[:, :, cut]), thirds[1] if shared_far else rows(far[1, :, :, cut])]
            one = (lax.broadcasted_iota(jnp.int32, (8, STEP), 0) == 0).astype(jnp.float32)
            blank = jnp.zeros((8, STEP), jnp.float32)
            lines = []
            for third in thirds:
                for i in range(vectors):
                    lines.append(mine[i:i + 1] * third)
                lines.append(third)
            left = jnp.concatenate(lines + [mine, one], axis=0).astype(jnp.bfloat16)
            side = partners + [one, blank]
            right = jnp.concatenate(side + side, axis=0).astype(jnp.bfloat16)
            acc[...] += lax.dot_general(
                left, right, (((1,), (1,)), ((), ())), preferred_element_type=jnp.float32)
            return carry

        lax.fori_loop(0, width // STEP, step, 0)

    ring = [own_copies(c) for c in range(CHUNKS)]
    hops = [hop_copies(c) for c in range(CHUNKS)]

    def start(copies):
        for copy in copies:
            copy.start()

    def arrive(copies):
        for copy in copies:
            copy.wait_recv()

    for c in range(min(2, CHUNKS)):
        start(ring[c])
    for c in range(CHUNKS + 1):
        if c < CHUNKS:
            arrive(ring[c])
            start(hops[c])
            if c + 2 < CHUNKS:
                start(ring[c + 2])
        if c > 0:
            arrive(hops[c - 1])
            contract(c - 1)

    lanes = acc.shape[1]
    packed = share // 2 * vectors
    first_half = lax.broadcasted_iota(jnp.int32, (packed, lanes), 1) < lanes // 2
    for plane in range(nr):
        base = plane * plane_rows
        for s in range(nf):
            slot = plane * nf + s
            at = base + s * share * vectors
            outgoing[slot, 0:packed] = jnp.where(
                first_half, acc[at:at + packed], acc[at + packed:at + 2 * packed])
            outgoing[slot, packed:packed + vectors] = acc[base + pair_rows:base + plane_rows]
            tail = nr * plane_rows
            line = packed + vectors
            outgoing[slot, line:line + share] = acc[tail + s * share:tail + (s + 1) * share]
            outgoing[slot, line + share:line + share + 2] = acc[tail + vectors:tail + vectors + 2]

    shares = []
    for offset in range(1, members):
        index, target = member(offset)
        copy = pltpu.make_async_remote_copy(
            src_ref=outgoing.at[index], dst_ref=incoming.at[offset],
            send_sem=table_send.at[offset], recv_sem=table_recv.at[offset],
            device_id=target, device_id_type=MESH)
        copy.start()
        shares.append(copy)
    total = outgoing[place]
    for offset, copy in enumerate(shares, 1):
        copy.wait_recv()
        total = total + incoming[offset]

    count = share * vectors // 2
    cols = o_ref.shape[1]
    source = lax.broadcasted_iota(jnp.int32, (lanes, lanes), 0)
    landing = lax.broadcasted_iota(jnp.int32, (lanes, lanes), 1)
    spread = jnp.where(landing < cols, landing // 2, cols // 2)

    def spread_out(value, start_lane):
        return jnp.dot(value, (source == spread + start_lane).astype(jnp.float32),
                       precision=lax.Precision.HIGHEST, preferred_element_type=jnp.float32)

    early = spread_out(total, 0)
    late = spread_out(total[0:packed], lanes // 2)
    pick = lax.broadcasted_iota(jnp.int32, (1, lanes), 1) % 2 == 1
    third_rows = early[packed:packed + vectors]
    line = packed + vectors
    third_sum = third_rows[:, cols:cols + 1]
    partner_sum = early[line + share:line + share + 1]
    twice = 2.0 * fields

    def gain(value):
        return 1.0 - value / (3.0 * fields)

    partner_counts = jnp.where(pick, partner_sum, twice - partner_sum)
    third_partner = jnp.where(pick, third_rows, 2.0 * third_sum - third_rows)
    scale_partner = gain(partner_counts) * (4.5 / (8.0 * fields))
    scale_third = [gain(twice - third_sum), gain(third_sum)]
    for i in range(share):
        from_value = early if i < share // 2 else late
        at = (i % (share // 2)) * vectors
        table = from_value[at:at + vectors]
        both = table[:, cols:cols + 1]
        own_row = early[line + i:line + i + 1]
        own_sum = own_row[:, cols:cols + 1]
        own_partner = jnp.where(pick, own_row, 2.0 * own_sum - own_row)
        t11 = jnp.where(pick, table, 2.0 * both - table)
        t01 = 2.0 * third_partner - t11
        t10 = 2.0 * own_partner - t11
        t00 = 4.0 * partner_counts - 2.0 * own_partner - t01
        scale_own = [gain(twice - own_sum), gain(own_sum)]
        for a, c, value in ((0, 0, t00), (0, 1, t01), (1, 0, t10), (1, 1, t11)):
            result = value * scale_own[a] * scale_third[c] * scale_partner
            o_ref[pl.ds((i * 2 + a) * vectors * 2 + c, vectors, stride=2), :] = result[:, :cols]

    for copies in ring + hops + [shares]:
        for copy in copies:
            copy.wait_send()


def solution(mesh):
    nv, nf, nr = mesh.shape["vec"], mesh.shape["field"], mesh.shape["rep"]

    def body(dosage):
        vectors, slice_width = dosage.shape
        fields = slice_width * nf
        groups = vectors // 8
        half = slice_width // nr
        share = vectors // nf
        members = nf * nr
        rows = nr * (vectors * vectors + vectors) + vectors + 8
        chunk_rows = share // 2 * vectors + vectors + share + 2
        block = pltpu.VMEM((groups, 8, half), jnp.bfloat16)
        dma = pltpu.SemaphoreType.DMA
        out = pl.pallas_call(
            functools.partial(kernel, nv, nf, nr, float(fields)),
            out_shape=jax.ShapeDtypeStruct((share * 2 * vectors * 2, 4 * vectors), jnp.float32),
            in_specs=[pl.BlockSpec(memory_space=pl.ANY)],
            out_specs=pl.BlockSpec(memory_space=pltpu.VMEM),
            scratch_shapes=[
                block, block, block,
                pltpu.VMEM((1 if nv == 4 else 2, groups, 8, half), jnp.bfloat16),
                pltpu.VMEM((rows, 128), jnp.float32),
                pltpu.VMEM((members, chunk_rows, 128), jnp.float32),
                pltpu.VMEM((members, chunk_rows, 128), jnp.float32),
                dma(()), dma((2, CHUNKS)), dma((2, CHUNKS)), dma((2, CHUNKS)), dma((2, CHUNKS)),
                dma((members,)), dma((members,)),
            ],
            compiler_params=pltpu.CompilerParams(
                collective_id=0, has_side_effects=True, vmem_limit_bytes=60 * 1024 * 1024),
        )(dosage.reshape(groups, 8, slice_width))
        return out.reshape(1, share, 2, vectors, 2, 4 * vectors)

    return jax.shard_map(
        body,
        mesh=mesh,
        in_specs=(P("vec", "field"),),
        out_specs=P("rep", ("vec", "field"), None, None, None, None),
        check_vma=False,
    )
```

```python
import functools

import jax
import jax.numpy as jnp
from jax import lax
from jax.experimental import pallas as pl
from jax.experimental.pallas import tpu as pltpu
from jax.sharding import PartitionSpec as P

MESH = pl.DeviceIdType.MESH
CHUNKS = 4
STEP = 512


def triples(mine, thirds, partners):
    vectors, width = mine.shape
    one = (lax.broadcasted_iota(jnp.int32, (8, width), 0) == 0).astype(jnp.float32)
    blank = jnp.zeros((8, width), jnp.float32)
    lines = []
    for third in thirds:
        for i in range(vectors):
            lines.append(mine[i:i + 1] * third)
        lines.append(third)
    left = jnp.concatenate(lines + [mine, one], axis=0).astype(jnp.bfloat16)
    side = partners + [one, blank]
    right = jnp.concatenate(side + side, axis=0).astype(jnp.bfloat16)
    return lax.dot_general(left, right, (((1,), (1,)), ((), ())), preferred_element_type=jnp.float32)


def pack(chunk, acc, plane, s, nr, share, vectors):
    lanes = acc.shape[1]
    pair_rows = vectors * vectors
    plane_rows = pair_rows + vectors
    packed = share // 2 * vectors
    first_half = lax.broadcasted_iota(jnp.int32, (packed, lanes), 1) < lanes // 2
    base = plane * plane_rows
    at = base + s * share * vectors
    tail = nr * plane_rows
    line = packed + vectors
    chunk[0:packed] = jnp.where(first_half, acc[at:at + packed], acc[at + packed:at + 2 * packed])
    chunk[packed:line] = acc[base + pair_rows:base + plane_rows]
    chunk[line:line + share] = acc[tail + s * share:tail + (s + 1) * share]
    chunk[line + share:line + share + 2] = acc[tail + vectors:tail + vectors + 2]


def finish(total, o_ref, fields, share, vectors):
    lanes = total.shape[1]
    packed = share // 2 * vectors
    cols = o_ref.shape[1]
    source = lax.broadcasted_iota(jnp.int32, (lanes, lanes), 0)
    landing = lax.broadcasted_iota(jnp.int32, (lanes, lanes), 1)
    spread = jnp.where(landing < cols, landing // 2, cols // 2)

    def spread_out(value, start_lane):
        return jnp.dot(value, (source == spread + start_lane).astype(jnp.float32),
                       precision=lax.Precision.HIGHEST, preferred_element_type=jnp.float32)

    early = spread_out(total, 0)
    late = spread_out(total[0:packed], lanes // 2)
    pick = lax.broadcasted_iota(jnp.int32, (1, lanes), 1) % 2 == 1
    third_rows = early[packed:packed + vectors]
    line = packed + vectors
    third_sum = third_rows[:, cols:cols + 1]
    partner_sum = early[line + share:line + share + 1]
    twice = 2.0 * fields

    def gain(value):
        return 1.0 - value / (3.0 * fields)

    partner_counts = jnp.where(pick, partner_sum, twice - partner_sum)
    third_partner = jnp.where(pick, third_rows, 2.0 * third_sum - third_rows)
    scale_partner = gain(partner_counts) * (4.5 / (8.0 * fields))
    scale_third = [gain(twice - third_sum), gain(third_sum)]
    for i in range(share):
        from_value = early if i < share // 2 else late
        at = (i % (share // 2)) * vectors
        table = from_value[at:at + vectors]
        both = table[:, cols:cols + 1]
        own_row = early[line + i:line + i + 1]
        own_sum = own_row[:, cols:cols + 1]
        own_partner = jnp.where(pick, own_row, 2.0 * own_sum - own_row)
        t11 = jnp.where(pick, table, 2.0 * both - table)
        t01 = 2.0 * third_partner - t11
        t10 = 2.0 * own_partner - t11
        t00 = 4.0 * partner_counts - 2.0 * own_partner - t01
        scale_own = [gain(twice - own_sum), gain(own_sum)]
        for a, c, value in ((0, 0, t00), (0, 1, t01), (1, 0, t10), (1, 1, t11)):
            result = value * scale_own[a] * scale_third[c] * scale_partner
            o_ref[pl.ds((i * 2 + a) * vectors * 2 + c, vectors, stride=2), :] = result[:, :cols]


def kernel(nv, nf, nr, fields, d_ref, o_ref, own, low, high, far, acc, outgoing, incoming,
           load_sem, ring_send, ring_recv, hop_send, hop_recv, table_send, table_recv):
    groups, _, half = own.shape
    vectors = groups * 8
    share = vectors // nf
    pair_rows = vectors * vectors
    plane_rows = pair_rows + vectors
    shared_far = far.shape[0] == 1
    width = half // CHUNKS
    members = nf * nr

    vec_at = lax.axis_index("vec")
    field_at = lax.axis_index("field")
    rep_at = lax.axis_index("rep")
    place = rep_at * nf + field_at
    above = {"vec": lax.rem(vec_at + 1, nv)}
    below = {"vec": lax.rem(vec_at + nv - 1, nv)}

    def member(offset):
        index = lax.rem(place + offset, members)
        return index, {"rep": index // nf, "field": lax.rem(index, nf)}

    load = pltpu.make_async_copy(
        d_ref.at[:, :, pl.ds(pl.multiple_of(rep_at * half, half), half)], own, load_sem
    )
    load.start()
    barrier = pltpu.get_barrier_semaphore()
    for target in (above, below):
        pl.semaphore_signal(barrier, inc=1, device_id=target, device_id_type=MESH)
    for offset in range(1, members):
        pl.semaphore_signal(barrier, inc=1, device_id=member(offset)[1], device_id_type=MESH)
    acc[...] = jnp.zeros_like(acc)
    load.wait()
    pl.semaphore_wait(barrier, members + 1)

    def own_copies(c):
        cut = pl.ds(c * width, width)
        return [
            pltpu.make_async_remote_copy(
                src_ref=own.at[:, :, cut], dst_ref=buffer.at[:, :, cut],
                send_sem=ring_send.at[way, c], recv_sem=ring_recv.at[way, c],
                device_id=target, device_id_type=MESH)
            for way, (buffer, target) in enumerate(((low, above), (high, below)))
        ]

    def hop_copies(c):
        copies = []
        for way, (buffer, target) in enumerate(((low, above), (high, below))):
            if shared_far:
                cut = pl.ds(c * width + way * (width // 2), width // 2)
                landing = far.at[0, :, :, cut]
            else:
                cut = pl.ds(c * width, width)
                landing = far.at[way, :, :, cut]
            copies.append(pltpu.make_async_remote_copy(
                src_ref=buffer.at[:, :, cut], dst_ref=landing,
                send_sem=hop_send.at[way, c], recv_sem=hop_recv.at[way, c],
                device_id=target, device_id_type=MESH))
        return copies

    def contract(c):
        def step(t, carry):
            cut = pl.ds(pl.multiple_of(c * width + t * STEP, STEP), STEP)

            def rows(block):
                return block.astype(jnp.float32).reshape(vectors, STEP)

            mine = rows(own[:, :, cut])
            thirds = [rows(low[:, :, cut]), rows(far[0, :, :, cut])]
            partners = [rows(high[:, :, cut]), thirds[1] if shared_far else rows(far[1, :, :, cut])]
            acc[...] += triples(mine, thirds, partners)
            return carry

        lax.fori_loop(0, width // STEP, step, 0)

    ring = [own_copies(c) for c in range(CHUNKS)]
    hops = [hop_copies(c) for c in range(CHUNKS)]

    def start(copies):
        for copy in copies:
            copy.start()

    def arrive(copies):
        for copy in copies:
            copy.wait_recv()

    for c in range(min(2, CHUNKS)):
        start(ring[c])
    for c in range(CHUNKS + 1):
        if c < CHUNKS:
            arrive(ring[c])
            start(hops[c])
            if c + 2 < CHUNKS:
                start(ring[c + 2])
        if c > 0:
            arrive(hops[c - 1])
            contract(c - 1)

    for plane in range(nr):
        for s in range(nf):
            pack(outgoing.at[plane * nf + s], acc, plane, s, nr, share, vectors)

    shares = []
    for offset in range(1, members):
        index, target = member(offset)
        copy = pltpu.make_async_remote_copy(
            src_ref=outgoing.at[index], dst_ref=incoming.at[offset],
            send_sem=table_send.at[offset], recv_sem=table_recv.at[offset],
            device_id=target, device_id_type=MESH)
        copy.start()
        shares.append(copy)
    total = outgoing[place]
    for offset, copy in enumerate(shares, 1):
        copy.wait_recv()
        total = total + incoming[offset]

    finish(total, o_ref, fields, share, vectors)
    for copies in ring + hops + [shares]:
        for copy in copies:
            copy.wait_send()


def quad_kernel(nf, nr, fields, d_ref, o_ref, blocks, ship, acc, outgoing, mates, summed, incoming,
                handoff, handed, load_sem, ring_send, ring_recv, hop_send,
                mate_sem, table_send, table_recv, hand_sem):
    _, groups, _, quarter = blocks.shape
    vectors = groups * 8
    share = vectors // nf
    columns = nf // 2
    seats = nr * columns
    width = quarter // CHUNKS

    z = lax.axis_index("vec")
    field_at = lax.axis_index("field")
    rep_at = lax.axis_index("rep")
    group = z // 2
    mate = z + 1 - 2 * lax.rem(z, 2)
    across = 2 - group
    across_end = 3 * (1 - group)
    middle = z == 1 + group
    core = lax.rem(field_at, 2)
    seat = rep_at * columns + field_at // 2
    partner = {"field": field_at + 1 - 2 * core}

    def seat_of(offset):
        index = lax.rem(seat + offset, seats)
        return index, {"rep": index // columns, "field": lax.rem(index, columns) * 2 + core}

    start_column = rep_at * 2 * quarter

    def part(g):
        return d_ref.at[:, :, pl.ds(pl.multiple_of(start_column + g * quarter, quarter), quarter)]

    loads = [pltpu.make_async_copy(part(1 - group), ship, load_sem.at[0]),
             pltpu.make_async_copy(part(group), blocks.at[z], load_sem.at[1])]
    for load in loads:
        load.start()
    barrier = pltpu.get_barrier_semaphore()
    for offset in range(1, 4):
        pl.semaphore_signal(barrier, inc=1, device_id={"vec": lax.rem(z + offset, 4)}, device_id_type=MESH)
    pl.semaphore_signal(barrier, inc=1, device_id=partner, device_id_type=MESH)
    for offset in range(1, seats):
        pl.semaphore_signal(barrier, inc=1, device_id=seat_of(offset)[1], device_id_type=MESH)
    acc[...] = jnp.zeros_like(acc)
    for load in loads:
        load.wait()
    pl.semaphore_wait(barrier, 3 + seats)

    def sent(source, block, c, send_sem, target):
        cut = pl.ds(c * width, width)
        return pltpu.make_async_remote_copy(
            src_ref=source.at[:, :, cut], dst_ref=blocks.at[block, :, :, cut],
            send_sem=send_sem, recv_sem=ring_recv.at[block, c],
            device_id={"vec": target}, device_id_type=MESH)

    firsts = []
    for c in range(CHUNKS):
        firsts.append(sent(ship, z, c, ring_send.at[0, c], across))
        firsts.append(sent(blocks.at[z], z, c, ring_send.at[1, c], mate))
    for copy in firsts:
        copy.start()

    def hop(k, c):
        block = (across, across_end)[k]
        return sent(blocks.at[block], block, c, hop_send.at[k, c], mate)

    def arrive(c, forward):
        for k in range(2):
            hop(k, c).wait_recv()
            if forward:
                hop(k, c).start()
        sent(blocks.at[mate], mate, c, hop_send.at[0, c], mate).wait_recv()

    def contract(c):
        def step(t, carry):
            cut = pl.ds(pl.multiple_of(c * width + t * STEP, STEP), STEP)
            mine, high, far, low = [
                blocks[lax.rem(z + k, 4), :, :, cut].astype(jnp.float32).reshape(vectors, STEP)
                for k in range(4)]
            acc[0] += triples(mine, [low, far], [high, far])
            acc[1] += triples(far, [high, mine], [low, mine])
            return carry

        lax.fori_loop(0, width // STEP, step, 0)

    pl.when(middle)(lambda: arrive(0, True))
    for c in range(CHUNKS):
        if c + 1 < CHUNKS:
            pl.when(middle)(functools.partial(arrive, c + 1, True))
        pl.when(jnp.logical_not(middle))(functools.partial(arrive, c, False))
        contract(c)

    for kind in range(2):
        for plane in range(nr):
            for s in range(nf):
                pack(outgoing.at[s % 2, plane * columns + s // 2, kind], acc.at[kind],
                     plane, s, nr, share, vectors)
    swap = pltpu.make_async_remote_copy(
        src_ref=outgoing.at[1 - core], dst_ref=mates, send_sem=mate_sem.at[0], recv_sem=mate_sem.at[1],
        device_id=partner, device_id_type=MESH)
    swap.start()
    swap.wait_recv()
    summed[...] = outgoing[core] + mates[...]
    shares = []
    for offset in range(1, seats):
        index, target = seat_of(offset)
        copy = pltpu.make_async_remote_copy(
            src_ref=summed.at[index], dst_ref=incoming.at[offset],
            send_sem=table_send.at[offset], recv_sem=table_recv.at[offset],
            device_id=target, device_id_type=MESH)
        copy.start()
        shares.append(copy)
    both = summed[seat]
    for offset, copy in enumerate(shares, 1):
        copy.wait_recv()
        both = both + incoming[offset]
    handoff[...] = both[1]
    hand = pltpu.make_async_remote_copy(
        src_ref=handoff, dst_ref=handed, send_sem=hand_sem.at[0], recv_sem=hand_sem.at[1],
        device_id={"vec": lax.rem(z + 2, 4)}, device_id_type=MESH)
    hand.start()
    hand.wait_recv()
    finish(both[0] + handed[...], o_ref, fields, share, vectors)

    for copy in firsts + shares + [swap, hand]:
        copy.wait_send()

    def drain():
        for c in range(CHUNKS):
            for k in range(2):
                hop(k, c).wait_send()

    pl.when(middle)(drain)


def quad_scratch(groups, quarter, rows, chunk_rows, seats):
    dma = pltpu.SemaphoreType.DMA
    return [
        pltpu.VMEM((4, groups, 8, quarter), jnp.bfloat16),
        pltpu.VMEM((groups, 8, quarter), jnp.bfloat16),
        pltpu.VMEM((2, rows, 128), jnp.float32),
        pltpu.VMEM((2, seats, 2, chunk_rows, 128), jnp.float32),
        pltpu.VMEM((seats, 2, chunk_rows, 128), jnp.float32),
        pltpu.VMEM((seats, 2, chunk_rows, 128), jnp.float32),
        pltpu.VMEM((seats, 2, chunk_rows, 128), jnp.float32),
        pltpu.VMEM((chunk_rows, 128), jnp.float32),
        pltpu.VMEM((chunk_rows, 128), jnp.float32),
        dma((2,)), dma((2, CHUNKS)), dma((4, CHUNKS)), dma((2, CHUNKS)),
        dma((2,)), dma((seats,)), dma((seats,)), dma((2,)),
    ]


def solution(mesh):
    nv, nf, nr = mesh.shape["vec"], mesh.shape["field"], mesh.shape["rep"]

    def body(dosage):
        vectors, slice_width = dosage.shape
        fields = slice_width * nf
        groups = vectors // 8
        half = slice_width // nr
        share = vectors // nf
        members = nf * nr
        rows = nr * (vectors * vectors + vectors) + vectors + 8
        chunk_rows = share // 2 * vectors + vectors + share + 2
        block = pltpu.VMEM((groups, 8, half), jnp.bfloat16)
        dma = pltpu.SemaphoreType.DMA
        if nv == 4:
            run = functools.partial(quad_kernel, nf, nr, float(fields))
            scratch = quad_scratch(groups, half // 2, rows, chunk_rows, members // 2)
        else:
            run = functools.partial(kernel, nv, nf, nr, float(fields))
            scratch = [
                block, block, block,
                pltpu.VMEM((1 if nv == 4 else 2, groups, 8, half), jnp.bfloat16),
                pltpu.VMEM((rows, 128), jnp.float32),
                pltpu.VMEM((members, chunk_rows, 128), jnp.float32),
                pltpu.VMEM((members, chunk_rows, 128), jnp.float32),
                dma(()), dma((2, CHUNKS)), dma((2, CHUNKS)), dma((2, CHUNKS)), dma((2, CHUNKS)),
                dma((members,)), dma((members,)),
            ]
        out = pl.pallas_call(
            run,
            out_shape=jax.ShapeDtypeStruct((share * 2 * vectors * 2, 4 * vectors), jnp.float32),
            in_specs=[pl.BlockSpec(memory_space=pl.ANY)],
            out_specs=pl.BlockSpec(memory_space=pltpu.VMEM),
            scratch_shapes=scratch,
            compiler_params=pltpu.CompilerParams(
                collective_id=0, has_side_effects=True, vmem_limit_bytes=60 * 1024 * 1024),
        )(dosage.reshape(groups, 8, slice_width))
        return out.reshape(1, share, 2, vectors, 2, 4 * vectors)

    return jax.shard_map(
        body,
        mesh=mesh,
        in_specs=(P("vec", "field"),),
        out_specs=P("rep", ("vec", "field"), None, None, None, None),
        check_vma=False,
    )
```

```python
import functools

import jax
import jax.numpy as jnp
from jax import lax
from jax.experimental import pallas as pl
from jax.experimental.pallas import tpu as pltpu
from jax.sharding import PartitionSpec as P

MESH = pl.DeviceIdType.MESH
CHUNKS = 4
STEP = 512


def triples(mine, thirds, partners):
    vectors, width = mine.shape
    one = (lax.broadcasted_iota(jnp.int32, (8, width), 0) == 0).astype(jnp.float32)
    blank = jnp.zeros((8, width), jnp.float32)
    lines = []
    for third in thirds:
        for i in range(vectors):
            lines.append(mine[i:i + 1] * third)
        lines.append(third)
    left = jnp.concatenate(lines + [mine, one], axis=0).astype(jnp.bfloat16)
    side = partners + [one, blank]
    right = jnp.concatenate(side + side, axis=0).astype(jnp.bfloat16)
    return lax.dot_general(left, right, (((1,), (1,)), ((), ())), preferred_element_type=jnp.float32)


def pack(chunk, acc, plane, s, nr, share, vectors):
    lanes = acc.shape[1]
    pair_rows = vectors * vectors
    plane_rows = pair_rows + vectors
    packed = share // 2 * vectors
    first_half = lax.broadcasted_iota(jnp.int32, (packed, lanes), 1) < lanes // 2
    base = plane * plane_rows
    at = base + s * share * vectors
    tail = nr * plane_rows
    line = packed + vectors
    chunk[0:packed] = jnp.where(first_half, acc[at:at + packed], acc[at + packed:at + 2 * packed])
    chunk[packed:line] = acc[base + pair_rows:base + plane_rows]
    chunk[line:line + share] = acc[tail + s * share:tail + (s + 1) * share]
    chunk[line + share:line + share + 2] = acc[tail + vectors:tail + vectors + 2]


def finish(total, o_ref, fields, share, vectors):
    lanes = total.shape[1]
    packed = share // 2 * vectors
    cols = o_ref.shape[1]
    source = lax.broadcasted_iota(jnp.int32, (lanes, lanes), 0)
    landing = lax.broadcasted_iota(jnp.int32, (lanes, lanes), 1)
    spread = jnp.where(landing < cols, landing // 2, cols // 2)

    def spread_out(value, start_lane):
        return jnp.dot(value, (source == spread + start_lane).astype(jnp.float32),
                       precision=lax.Precision.HIGHEST, preferred_element_type=jnp.float32)

    early = spread_out(total, 0)
    late = spread_out(total[0:packed], lanes // 2)
    pick = lax.broadcasted_iota(jnp.int32, (1, lanes), 1) % 2 == 1
    third_rows = early[packed:packed + vectors]
    line = packed + vectors
    third_sum = third_rows[:, cols:cols + 1]
    partner_sum = early[line + share:line + share + 1]
    twice = 2.0 * fields

    def gain(value):
        return 1.0 - value / (3.0 * fields)

    partner_counts = jnp.where(pick, partner_sum, twice - partner_sum)
    third_partner = jnp.where(pick, third_rows, 2.0 * third_sum - third_rows)
    scale_partner = gain(partner_counts) * (4.5 / (8.0 * fields))
    scale_third = [gain(twice - third_sum), gain(third_sum)]
    for i in range(share):
        from_value = early if i < share // 2 else late
        at = (i % (share // 2)) * vectors
        table = from_value[at:at + vectors]
        both = table[:, cols:cols + 1]
        own_row = early[line + i:line + i + 1]
        own_sum = own_row[:, cols:cols + 1]
        own_partner = jnp.where(pick, own_row, 2.0 * own_sum - own_row)
        t11 = jnp.where(pick, table, 2.0 * both - table)
        t01 = 2.0 * third_partner - t11
        t10 = 2.0 * own_partner - t11
        t00 = 4.0 * partner_counts - 2.0 * own_partner - t01
        scale_own = [gain(twice - own_sum), gain(own_sum)]
        for a, c, value in ((0, 0, t00), (0, 1, t01), (1, 0, t10), (1, 1, t11)):
            result = value * scale_own[a] * scale_third[c] * scale_partner
            o_ref[pl.ds((i * 2 + a) * vectors * 2 + c, vectors, stride=2), :] = result[:, :cols]


def kernel(nv, nf, nr, fields, d_ref, o_ref, own, low, high, far, acc, outgoing, incoming,
           load_sem, ring_send, ring_recv, hop_send, hop_recv, table_send, table_recv):
    groups, _, half = own.shape
    vectors = groups * 8
    share = vectors // nf
    pair_rows = vectors * vectors
    plane_rows = pair_rows + vectors
    shared_far = far.shape[0] == 1
    width = half // CHUNKS
    members = nf * nr

    vec_at = lax.axis_index("vec")
    field_at = lax.axis_index("field")
    rep_at = lax.axis_index("rep")
    place = rep_at * nf + field_at
    above = {"vec": lax.rem(vec_at + 1, nv)}
    below = {"vec": lax.rem(vec_at + nv - 1, nv)}

    def member(offset):
        index = lax.rem(place + offset, members)
        return index, {"rep": index // nf, "field": lax.rem(index, nf)}

    load = pltpu.make_async_copy(
        d_ref.at[:, :, pl.ds(pl.multiple_of(rep_at * half, half), half)], own, load_sem
    )
    load.start()
    barrier = pltpu.get_barrier_semaphore()
    for target in (above, below):
        pl.semaphore_signal(barrier, inc=1, device_id=target, device_id_type=MESH)
    for offset in range(1, members):
        pl.semaphore_signal(barrier, inc=1, device_id=member(offset)[1], device_id_type=MESH)
    acc[...] = jnp.zeros_like(acc)
    load.wait()
    pl.semaphore_wait(barrier, members + 1)

    def own_copies(c):
        cut = pl.ds(c * width, width)
        return [
            pltpu.make_async_remote_copy(
                src_ref=own.at[:, :, cut], dst_ref=buffer.at[:, :, cut],
                send_sem=ring_send.at[way, c], recv_sem=ring_recv.at[way, c],
                device_id=target, device_id_type=MESH)
            for way, (buffer, target) in enumerate(((low, above), (high, below)))
        ]

    def hop_copies(c):
        copies = []
        for way, (buffer, target) in enumerate(((low, above), (high, below))):
            if shared_far:
                cut = pl.ds(c * width + way * (width // 2), width // 2)
                landing = far.at[0, :, :, cut]
            else:
                cut = pl.ds(c * width, width)
                landing = far.at[way, :, :, cut]
            copies.append(pltpu.make_async_remote_copy(
                src_ref=buffer.at[:, :, cut], dst_ref=landing,
                send_sem=hop_send.at[way, c], recv_sem=hop_recv.at[way, c],
                device_id=target, device_id_type=MESH))
        return copies

    def contract(c):
        def step(t, carry):
            cut = pl.ds(pl.multiple_of(c * width + t * STEP, STEP), STEP)

            def rows(block):
                return block.astype(jnp.float32).reshape(vectors, STEP)

            mine = rows(own[:, :, cut])
            thirds = [rows(low[:, :, cut]), rows(far[0, :, :, cut])]
            partners = [rows(high[:, :, cut]), thirds[1] if shared_far else rows(far[1, :, :, cut])]
            acc[...] += triples(mine, thirds, partners)
            return carry

        lax.fori_loop(0, width // STEP, step, 0)

    ring = [own_copies(c) for c in range(CHUNKS)]
    hops = [hop_copies(c) for c in range(CHUNKS)]

    def start(copies):
        for copy in copies:
            copy.start()

    def arrive(copies):
        for copy in copies:
            copy.wait_recv()

    for c in range(min(2, CHUNKS)):
        start(ring[c])
    for c in range(CHUNKS + 1):
        if c < CHUNKS:
            arrive(ring[c])
            start(hops[c])
            if c + 2 < CHUNKS:
                start(ring[c + 2])
        if c > 0:
            arrive(hops[c - 1])
            contract(c - 1)

    for plane in range(nr):
        for s in range(nf):
            pack(outgoing.at[plane * nf + s], acc, plane, s, nr, share, vectors)

    shares = []
    for offset in range(1, members):
        index, target = member(offset)
        copy = pltpu.make_async_remote_copy(
            src_ref=outgoing.at[index], dst_ref=incoming.at[offset],
            send_sem=table_send.at[offset], recv_sem=table_recv.at[offset],
            device_id=target, device_id_type=MESH)
        copy.start()
        shares.append(copy)
    total = outgoing[place]
    for offset, copy in enumerate(shares, 1):
        copy.wait_recv()
        total = total + incoming[offset]

    finish(total, o_ref, fields, share, vectors)
    for copies in ring + hops + [shares]:
        for copy in copies:
            copy.wait_send()


def quad_kernel(nf, nr, fields, d_ref, o_ref, blocks, ship, acc, outgoing, mates, summed, incoming,
                handoff, handed, load_sem, ring_send, ring_recv, hop_send,
                mate_sem, table_send, table_recv, hand_sem):
    _, groups, _, quarter = blocks.shape
    vectors = groups * 8
    share = vectors // nf
    columns = nf // 2
    seats = nr * columns
    width = quarter // CHUNKS

    z = lax.axis_index("vec")
    field_at = lax.axis_index("field")
    rep_at = lax.axis_index("rep")
    group = z // 2
    mate = z + 1 - 2 * lax.rem(z, 2)
    across = 2 - group
    across_end = 3 * (1 - group)
    middle = z == 1 + group
    core = lax.rem(field_at, 2)
    seat = rep_at * columns + field_at // 2
    partner = {"field": field_at + 1 - 2 * core}

    def seat_of(offset):
        index = lax.rem(seat + offset, seats)
        return index, {"rep": index // columns, "field": lax.rem(index, columns) * 2 + core}

    start_column = rep_at * 2 * quarter

    def part(g):
        return d_ref.at[:, :, pl.ds(pl.multiple_of(start_column + g * quarter, quarter), quarter)]

    loads = [pltpu.make_async_copy(part(1 - group), ship, load_sem.at[0]),
             pltpu.make_async_copy(part(group), blocks.at[z], load_sem.at[1])]
    for load in loads:
        load.start()
    barrier = pltpu.get_barrier_semaphore()
    for offset in range(1, 4):
        pl.semaphore_signal(barrier, inc=1, device_id={"vec": lax.rem(z + offset, 4)}, device_id_type=MESH)
    pl.semaphore_signal(barrier, inc=1, device_id=partner, device_id_type=MESH)
    for offset in range(1, seats):
        pl.semaphore_signal(barrier, inc=1, device_id=seat_of(offset)[1], device_id_type=MESH)
    acc[...] = jnp.zeros_like(acc)
    for load in loads:
        load.wait()
    pl.semaphore_wait(barrier, 3 + seats)

    def sent(source, block, c, send_sem, target):
        cut = pl.ds(c * width, width)
        return pltpu.make_async_remote_copy(
            src_ref=source.at[:, :, cut], dst_ref=blocks.at[block, :, :, cut],
            send_sem=send_sem, recv_sem=ring_recv.at[block, c],
            device_id={"vec": target}, device_id_type=MESH)

    firsts = []
    for c in range(CHUNKS):
        firsts.append(sent(ship, z, c, ring_send.at[0, c], across))
        firsts.append(sent(blocks.at[z], z, c, ring_send.at[1, c], mate))
    for copy in firsts:
        copy.start()

    def hop(k, c):
        block = (across, across_end)[k]
        return sent(blocks.at[block], block, c, hop_send.at[k, c], mate)

    def arrive(c, forward):
        for k in range(2):
            hop(k, c).wait_recv()
            if forward:
                hop(k, c).start()
        sent(blocks.at[mate], mate, c, hop_send.at[0, c], mate).wait_recv()

    def contract(c, kinds):
        def step(t, carry):
            cut = pl.ds(pl.multiple_of(c * width + t * STEP, STEP), STEP)
            mine, high, far, low = [
                blocks[lax.rem(z + k, 4), :, :, cut].astype(jnp.float32).reshape(vectors, STEP)
                for k in range(4)]
            if 0 in kinds:
                acc[0] += triples(mine, [low, far], [high, far])
            if 1 in kinds:
                acc[1] += triples(far, [high, mine], [low, mine])
            return carry

        lax.fori_loop(0, width // STEP, step, 0)

    pl.when(middle)(lambda: arrive(0, True))
    for c in range(CHUNKS):
        if c + 1 < CHUNKS:
            pl.when(middle)(functools.partial(arrive, c + 1, True))
        pl.when(jnp.logical_not(middle))(functools.partial(arrive, c, False))
        if c + 1 < CHUNKS:
            contract(c, (0, 1))

    swaps = {}
    for kind in (1, 0):
        contract(CHUNKS - 1, (kind,))
        for plane in range(nr):
            for s in range(nf):
                pack(outgoing.at[s % 2, kind, plane * columns + s // 2], acc.at[kind],
                     plane, s, nr, share, vectors)
        swaps[kind] = pltpu.make_async_remote_copy(
            src_ref=outgoing.at[1 - core, kind], dst_ref=mates.at[kind],
            send_sem=mate_sem.at[0, kind], recv_sem=mate_sem.at[1, kind],
            device_id=partner, device_id_type=MESH)
        swaps[kind].start()

    shares = {}
    for kind in (1, 0):
        swaps[kind].wait_recv()
        summed[kind] = outgoing[core, kind] + mates[kind]
        shares[kind] = []
        for offset in range(1, seats):
            index, target = seat_of(offset)
            copy = pltpu.make_async_remote_copy(
                src_ref=summed.at[kind, index], dst_ref=incoming.at[kind, offset],
                send_sem=table_send.at[kind, offset], recv_sem=table_recv.at[kind, offset],
                device_id=target, device_id_type=MESH)
            copy.start()
            shares[kind].append(copy)

    def gathered(kind):
        total = summed[kind, seat]
        for offset, copy in enumerate(shares[kind], 1):
            copy.wait_recv()
            total = total + incoming[kind, offset]
        return total

    handoff[...] = gathered(1)
    hand = pltpu.make_async_remote_copy(
        src_ref=handoff, dst_ref=handed, send_sem=hand_sem.at[0], recv_sem=hand_sem.at[1],
        device_id={"vec": lax.rem(z + 2, 4)}, device_id_type=MESH)
    hand.start()
    kept = gathered(0)
    hand.wait_recv()
    finish(kept + handed[...], o_ref, fields, share, vectors)

    for copy in firsts + shares[0] + shares[1] + [swaps[0], swaps[1], hand]:
        copy.wait_send()

    def drain():
        for c in range(CHUNKS):
            for k in range(2):
                hop(k, c).wait_send()

    pl.when(middle)(drain)


def quad_scratch(groups, quarter, rows, chunk_rows, seats):
    dma = pltpu.SemaphoreType.DMA
    return [
        pltpu.VMEM((4, groups, 8, quarter), jnp.bfloat16),
        pltpu.VMEM((groups, 8, quarter), jnp.bfloat16),
        pltpu.VMEM((2, rows, 128), jnp.float32),
        pltpu.VMEM((2, 2, seats, chunk_rows, 128), jnp.float32),
        pltpu.VMEM((2, seats, chunk_rows, 128), jnp.float32),
        pltpu.VMEM((2, seats, chunk_rows, 128), jnp.float32),
        pltpu.VMEM((2, seats, chunk_rows, 128), jnp.float32),
        pltpu.VMEM((chunk_rows, 128), jnp.float32),
        pltpu.VMEM((chunk_rows, 128), jnp.float32),
        dma((2,)), dma((2, CHUNKS)), dma((4, CHUNKS)), dma((2, CHUNKS)),
        dma((2, 2)), dma((2, seats)), dma((2, seats)), dma((2,)),
    ]


def solution(mesh):
    nv, nf, nr = mesh.shape["vec"], mesh.shape["field"], mesh.shape["rep"]

    def body(dosage):
        vectors, slice_width = dosage.shape
        fields = slice_width * nf
        groups = vectors // 8
        half = slice_width // nr
        share = vectors // nf
        members = nf * nr
        rows = nr * (vectors * vectors + vectors) + vectors + 8
        chunk_rows = share // 2 * vectors + vectors + share + 2
        block = pltpu.VMEM((groups, 8, half), jnp.bfloat16)
        dma = pltpu.SemaphoreType.DMA
        if nv == 4:
            run = functools.partial(quad_kernel, nf, nr, float(fields))
            scratch = quad_scratch(groups, half // 2, rows, chunk_rows, members // 2)
        else:
            run = functools.partial(kernel, nv, nf, nr, float(fields))
            scratch = [
                block, block, block,
                pltpu.VMEM((1 if nv == 4 else 2, groups, 8, half), jnp.bfloat16),
                pltpu.VMEM((rows, 128), jnp.float32),
                pltpu.VMEM((members, chunk_rows, 128), jnp.float32),
                pltpu.VMEM((members, chunk_rows, 128), jnp.float32),
                dma(()), dma((2, CHUNKS)), dma((2, CHUNKS)), dma((2, CHUNKS)), dma((2, CHUNKS)),
                dma((members,)), dma((members,)),
            ]
        out = pl.pallas_call(
            run,
            out_shape=jax.ShapeDtypeStruct((share * 2 * vectors * 2, 4 * vectors), jnp.float32),
            in_specs=[pl.BlockSpec(memory_space=pl.ANY)],
            out_specs=pl.BlockSpec(memory_space=pltpu.VMEM),
            scratch_shapes=scratch,
            compiler_params=pltpu.CompilerParams(
                collective_id=0, has_side_effects=True, vmem_limit_bytes=60 * 1024 * 1024),
        )(dosage.reshape(groups, 8, slice_width))
        return out.reshape(1, share, 2, vectors, 2, 4 * vectors)

    return jax.shard_map(
        body,
        mesh=mesh,
        in_specs=(P("vec", "field"),),
        out_specs=P("rep", ("vec", "field"), None, None, None, None),
        check_vma=False,
    )
```

```python
import functools

import jax
import jax.numpy as jnp
from jax import lax
from jax.experimental import pallas as pl
from jax.experimental.pallas import tpu as pltpu
from jax.sharding import PartitionSpec as P

MESH = pl.DeviceIdType.MESH
CHUNKS = 4
STEP = 512


def triples(mine, thirds, partners):
    vectors, width = mine.shape
    one = (lax.broadcasted_iota(jnp.int32, (8, width), 0) == 0).astype(jnp.float32)
    blank = jnp.zeros((8, width), jnp.float32)
    lines = []
    for third in thirds:
        for i in range(vectors):
            lines.append(mine[i:i + 1] * third)
        lines.append(third)
    left = jnp.concatenate(lines + [mine, one], axis=0).astype(jnp.bfloat16)
    side = partners + [one, blank]
    right = jnp.concatenate(side + side, axis=0).astype(jnp.bfloat16)
    return lax.dot_general(left, right, (((1,), (1,)), ((), ())), preferred_element_type=jnp.float32)


def pack(chunk, acc, plane, s, nr, share, vectors):
    lanes = acc.shape[1]
    pair_rows = vectors * vectors
    plane_rows = pair_rows + vectors
    packed = share // 2 * vectors
    first_half = lax.broadcasted_iota(jnp.int32, (packed, lanes), 1) < lanes // 2
    base = plane * plane_rows
    at = base + s * share * vectors
    tail = nr * plane_rows
    half = vectors // 2
    line = packed + half
    thirds = base + pair_rows
    chunk[0:packed] = jnp.where(first_half, acc[at:at + packed], acc[at + packed:at + 2 * packed])
    chunk[packed:line] = jnp.where(
        first_half[0:half], acc[thirds:thirds + half], acc[thirds + half:thirds + vectors])
    chunk[line:line + share] = acc[tail + s * share:tail + (s + 1) * share]
    chunk[line + share:line + share + 2] = acc[tail + vectors:tail + vectors + 2]


def finish(total, o_ref, fields, share, vectors):
    lanes = total.shape[1]
    packed = share // 2 * vectors
    line = packed + vectors // 2
    cols = o_ref.shape[1]
    source = lax.broadcasted_iota(jnp.int32, (lanes, lanes), 0)
    landing = lax.broadcasted_iota(jnp.int32, (lanes, lanes), 1)
    spread = jnp.where(landing < cols, landing // 2, cols // 2)

    def spread_out(value, start_lane):
        return jnp.dot(value, (source == spread + start_lane).astype(jnp.float32),
                       precision=lax.Precision.HIGHEST, preferred_element_type=jnp.float32)

    early = spread_out(total, 0)
    late = spread_out(total[0:line], lanes // 2)
    pick = lax.broadcasted_iota(jnp.int32, (1, lanes), 1) % 2 == 1
    third_rows = jnp.concatenate([early[packed:line], late[packed:line]], axis=0)
    third_sum = third_rows[:, cols:cols + 1]
    partner_sum = early[line + share:line + share + 1]
    twice = 2.0 * fields

    def gain(value):
        return 1.0 - value / (3.0 * fields)

    partner_counts = jnp.where(pick, partner_sum, twice - partner_sum)
    third_partner = jnp.where(pick, third_rows, 2.0 * third_sum - third_rows)
    scale_partner = gain(partner_counts) * (4.5 / (8.0 * fields))
    scale_third = [gain(twice - third_sum), gain(third_sum)]
    for i in range(share):
        from_value = early if i < share // 2 else late
        at = (i % (share // 2)) * vectors
        table = from_value[at:at + vectors]
        both = table[:, cols:cols + 1]
        own_row = early[line + i:line + i + 1]
        own_sum = own_row[:, cols:cols + 1]
        own_partner = jnp.where(pick, own_row, 2.0 * own_sum - own_row)
        t11 = jnp.where(pick, table, 2.0 * both - table)
        t01 = 2.0 * third_partner - t11
        t10 = 2.0 * own_partner - t11
        t00 = 4.0 * partner_counts - 2.0 * own_partner - t01
        scale_own = [gain(twice - own_sum), gain(own_sum)]
        for a, c, value in ((0, 0, t00), (0, 1, t01), (1, 0, t10), (1, 1, t11)):
            result = value * scale_own[a] * scale_third[c] * scale_partner
            o_ref[pl.ds((i * 2 + a) * vectors * 2 + c, vectors, stride=2), :] = result[:, :cols]


def finish_kernel(fields, share, vectors, total_ref, o_ref):
    finish(total_ref[...], o_ref, fields, share, vectors)


def kernel(nv, nf, nr, fields, d_ref, o_ref, own, low, high, far, acc, outgoing, incoming,
           load_sem, ring_send, ring_recv, hop_send, hop_recv, table_send, table_recv):
    groups, _, half = own.shape
    vectors = groups * 8
    share = vectors // nf
    pair_rows = vectors * vectors
    plane_rows = pair_rows + vectors
    shared_far = far.shape[0] == 1
    width = half // CHUNKS
    members = nf * nr

    vec_at = lax.axis_index("vec")
    field_at = lax.axis_index("field")
    rep_at = lax.axis_index("rep")
    place = rep_at * nf + field_at
    above = {"vec": lax.rem(vec_at + 1, nv)}
    below = {"vec": lax.rem(vec_at + nv - 1, nv)}

    def member(offset):
        index = lax.rem(place + offset, members)
        return index, {"rep": index // nf, "field": lax.rem(index, nf)}

    load = pltpu.make_async_copy(
        d_ref.at[:, :, pl.ds(pl.multiple_of(rep_at * half, half), half)], own, load_sem
    )
    load.start()
    barrier = pltpu.get_barrier_semaphore()
    for target in (above, below):
        pl.semaphore_signal(barrier, inc=1, device_id=target, device_id_type=MESH)
    for offset in range(1, members):
        pl.semaphore_signal(barrier, inc=1, device_id=member(offset)[1], device_id_type=MESH)
    acc[...] = jnp.zeros_like(acc)
    load.wait()
    pl.semaphore_wait(barrier, members + 1)

    def own_copies(c):
        cut = pl.ds(c * width, width)
        return [
            pltpu.make_async_remote_copy(
                src_ref=own.at[:, :, cut], dst_ref=buffer.at[:, :, cut],
                send_sem=ring_send.at[way, c], recv_sem=ring_recv.at[way, c],
                device_id=target, device_id_type=MESH)
            for way, (buffer, target) in enumerate(((low, above), (high, below)))
        ]

    def hop_copies(c):
        copies = []
        for way, (buffer, target) in enumerate(((low, above), (high, below))):
            if shared_far:
                cut = pl.ds(c * width + way * (width // 2), width // 2)
                landing = far.at[0, :, :, cut]
            else:
                cut = pl.ds(c * width, width)
                landing = far.at[way, :, :, cut]
            copies.append(pltpu.make_async_remote_copy(
                src_ref=buffer.at[:, :, cut], dst_ref=landing,
                send_sem=hop_send.at[way, c], recv_sem=hop_recv.at[way, c],
                device_id=target, device_id_type=MESH))
        return copies

    def contract(c):
        def step(t, carry):
            cut = pl.ds(pl.multiple_of(c * width + t * STEP, STEP), STEP)

            def rows(block):
                return block.astype(jnp.float32).reshape(vectors, STEP)

            mine = rows(own[:, :, cut])
            thirds = [rows(low[:, :, cut]), rows(far[0, :, :, cut])]
            partners = [rows(high[:, :, cut]), thirds[1] if shared_far else rows(far[1, :, :, cut])]
            acc[...] += triples(mine, thirds, partners)
            return carry

        lax.fori_loop(0, width // STEP, step, 0)

    ring = [own_copies(c) for c in range(CHUNKS)]
    hops = [hop_copies(c) for c in range(CHUNKS)]

    def start(copies):
        for copy in copies:
            copy.start()

    def arrive(copies):
        for copy in copies:
            copy.wait_recv()

    for c in range(min(2, CHUNKS)):
        start(ring[c])
    for c in range(CHUNKS + 1):
        if c < CHUNKS:
            arrive(ring[c])
            start(hops[c])
            if c + 2 < CHUNKS:
                start(ring[c + 2])
        if c > 0:
            arrive(hops[c - 1])
            contract(c - 1)

    for plane in range(nr):
        for s in range(nf):
            pack(outgoing.at[plane * nf + s], acc, plane, s, nr, share, vectors)

    shares = []
    for offset in range(1, members):
        index, target = member(offset)
        copy = pltpu.make_async_remote_copy(
            src_ref=outgoing.at[index], dst_ref=incoming.at[offset],
            send_sem=table_send.at[offset], recv_sem=table_recv.at[offset],
            device_id=target, device_id_type=MESH)
        copy.start()
        shares.append(copy)
    total = outgoing[place]
    for offset, copy in enumerate(shares, 1):
        copy.wait_recv()
        total = total + incoming[offset]

    o_ref[...] = total
    for copies in ring + hops + [shares]:
        for copy in copies:
            copy.wait_send()


def quad_kernel(nf, nr, fields, d_ref, o_ref, blocks, ship, acc, outgoing, mates, summed, incoming,
                handoff, handed, load_sem, ring_send, ring_recv, hop_send,
                mate_sem, table_send, table_recv, hand_sem):
    _, groups, _, quarter = blocks.shape
    vectors = groups * 8
    share = vectors // nf
    columns = nf // 2
    seats = nr * columns
    width = quarter // CHUNKS

    z = lax.axis_index("vec")
    field_at = lax.axis_index("field")
    rep_at = lax.axis_index("rep")
    group = z // 2
    mate = z + 1 - 2 * lax.rem(z, 2)
    across = 2 - group
    across_end = 3 * (1 - group)
    middle = z == 1 + group
    core = lax.rem(field_at, 2)
    seat = rep_at * columns + field_at // 2
    partner = {"field": field_at + 1 - 2 * core}

    def seat_of(offset):
        index = lax.rem(seat + offset, seats)
        return index, {"rep": index // columns, "field": lax.rem(index, columns) * 2 + core}

    start_column = rep_at * 2 * quarter

    def part(g):
        return d_ref.at[:, :, pl.ds(pl.multiple_of(start_column + g * quarter, quarter), quarter)]

    loads = [pltpu.make_async_copy(part(1 - group), ship, load_sem.at[0]),
             pltpu.make_async_copy(part(group), blocks.at[z], load_sem.at[1])]
    for load in loads:
        load.start()
    barrier = pltpu.get_barrier_semaphore()
    for offset in range(1, 4):
        pl.semaphore_signal(barrier, inc=1, device_id={"vec": lax.rem(z + offset, 4)}, device_id_type=MESH)
    pl.semaphore_signal(barrier, inc=1, device_id=partner, device_id_type=MESH)
    for offset in range(1, seats):
        pl.semaphore_signal(barrier, inc=1, device_id=seat_of(offset)[1], device_id_type=MESH)
    acc[...] = jnp.zeros_like(acc)
    for load in loads:
        load.wait()
    pl.semaphore_wait(barrier, 3 + seats)

    def sent(source, block, c, send_sem, target):
        cut = pl.ds(c * width, width)
        return pltpu.make_async_remote_copy(
            src_ref=source.at[:, :, cut], dst_ref=blocks.at[block, :, :, cut],
            send_sem=send_sem, recv_sem=ring_recv.at[block, c],
            device_id={"vec": target}, device_id_type=MESH)

    firsts = []
    for c in range(CHUNKS):
        firsts.append(sent(ship, z, c, ring_send.at[0, c], across))
        firsts.append(sent(blocks.at[z], z, c, ring_send.at[1, c], mate))
    for copy in firsts:
        copy.start()

    def hop(k, c):
        block = (across, across_end)[k]
        return sent(blocks.at[block], block, c, hop_send.at[k, c], mate)

    def arrive(c, forward):
        for k in range(2):
            hop(k, c).wait_recv()
            if forward:
                hop(k, c).start()
        sent(blocks.at[mate], mate, c, hop_send.at[0, c], mate).wait_recv()

    def contract(c, kinds):
        def step(t, carry):
            cut = pl.ds(pl.multiple_of(c * width + t * STEP, STEP), STEP)
            mine, high, far, low = [
                blocks[lax.rem(z + k, 4), :, :, cut].astype(jnp.float32).reshape(vectors, STEP)
                for k in range(4)]
            if 0 in kinds:
                acc[0] += triples(mine, [low, far], [high, far])
            if 1 in kinds:
                acc[1] += triples(far, [high, mine], [low, mine])
            return carry

        lax.fori_loop(0, width // STEP, step, 0)

    pl.when(middle)(lambda: arrive(0, True))
    for c in range(CHUNKS):
        if c + 1 < CHUNKS:
            pl.when(middle)(functools.partial(arrive, c + 1, True))
        pl.when(jnp.logical_not(middle))(functools.partial(arrive, c, False))
        if c + 1 < CHUNKS:
            contract(c, (0, 1))

    swaps = {}
    for kind in (1, 0):
        contract(CHUNKS - 1, (kind,))
        for plane in range(nr):
            for s in range(nf):
                pack(outgoing.at[s % 2, kind, plane * columns + s // 2], acc.at[kind],
                     plane, s, nr, share, vectors)
        swaps[kind] = pltpu.make_async_remote_copy(
            src_ref=outgoing.at[1 - core, kind], dst_ref=mates.at[kind],
            send_sem=mate_sem.at[0, kind], recv_sem=mate_sem.at[1, kind],
            device_id=partner, device_id_type=MESH)
        swaps[kind].start()

    shares = {}
    for kind in (1, 0):
        swaps[kind].wait_recv()
        summed[kind] = outgoing[core, kind] + mates[kind]
        shares[kind] = []
        for offset in range(1, seats):
            index, target = seat_of(offset)
            copy = pltpu.make_async_remote_copy(
                src_ref=summed.at[kind, index], dst_ref=incoming.at[kind, offset],
                send_sem=table_send.at[kind, offset], recv_sem=table_recv.at[kind, offset],
                device_id=target, device_id_type=MESH)
            copy.start()
            shares[kind].append(copy)

    def gathered(kind):
        total = summed[kind, seat]
        for offset, copy in enumerate(shares[kind], 1):
            copy.wait_recv()
            total = total + incoming[kind, offset]
        return total

    handoff[...] = gathered(1)
    hand = pltpu.make_async_remote_copy(
        src_ref=handoff, dst_ref=handed, send_sem=hand_sem.at[0], recv_sem=hand_sem.at[1],
        device_id={"vec": lax.rem(z + 2, 4)}, device_id_type=MESH)
    hand.start()
    kept = gathered(0)
    hand.wait_recv()
    o_ref[...] = kept + handed[...]

    for copy in firsts + shares[0] + shares[1] + [swaps[0], swaps[1], hand]:
        copy.wait_send()

    def drain():
        for c in range(CHUNKS):
            for k in range(2):
                hop(k, c).wait_send()

    pl.when(middle)(drain)


def quad_scratch(groups, quarter, rows, chunk_rows, seats):
    dma = pltpu.SemaphoreType.DMA
    return [
        pltpu.VMEM((4, groups, 8, quarter), jnp.bfloat16),
        pltpu.VMEM((groups, 8, quarter), jnp.bfloat16),
        pltpu.VMEM((2, rows, 128), jnp.float32),
        pltpu.VMEM((2, 2, seats, chunk_rows, 128), jnp.float32),
        pltpu.VMEM((2, seats, chunk_rows, 128), jnp.float32),
        pltpu.VMEM((2, seats, chunk_rows, 128), jnp.float32),
        pltpu.VMEM((2, seats, chunk_rows, 128), jnp.float32),
        pltpu.VMEM((chunk_rows, 128), jnp.float32),
        pltpu.VMEM((chunk_rows, 128), jnp.float32),
        dma((2,)), dma((2, CHUNKS)), dma((4, CHUNKS)), dma((2, CHUNKS)),
        dma((2, 2)), dma((2, seats)), dma((2, seats)), dma((2,)),
    ]


def solution(mesh):
    nv, nf, nr = mesh.shape["vec"], mesh.shape["field"], mesh.shape["rep"]

    def body(dosage):
        vectors, slice_width = dosage.shape
        fields = slice_width * nf
        groups = vectors // 8
        half = slice_width // nr
        share = vectors // nf
        members = nf * nr
        rows = nr * (vectors * vectors + vectors) + vectors + 8
        chunk_rows = share // 2 * vectors + vectors // 2 + share + 2
        block = pltpu.VMEM((groups, 8, half), jnp.bfloat16)
        dma = pltpu.SemaphoreType.DMA
        if nv == 4:
            run = functools.partial(quad_kernel, nf, nr, float(fields))
            scratch = quad_scratch(groups, half // 2, rows, chunk_rows, members // 2)
        else:
            run = functools.partial(kernel, nv, nf, nr, float(fields))
            scratch = [
                block, block, block,
                pltpu.VMEM((1 if nv == 4 else 2, groups, 8, half), jnp.bfloat16),
                pltpu.VMEM((rows, 128), jnp.float32),
                pltpu.VMEM((members, chunk_rows, 128), jnp.float32),
                pltpu.VMEM((members, chunk_rows, 128), jnp.float32),
                dma(()), dma((2, CHUNKS)), dma((2, CHUNKS)), dma((2, CHUNKS)), dma((2, CHUNKS)),
                dma((members,)), dma((members,)),
            ]
        total = pl.pallas_call(
            run,
            out_shape=jax.ShapeDtypeStruct((chunk_rows, 128), jnp.float32),
            in_specs=[pl.BlockSpec(memory_space=pl.ANY)],
            out_specs=pl.BlockSpec(memory_space=pltpu.VMEM),
            scratch_shapes=scratch,
            compiler_params=pltpu.CompilerParams(
                collective_id=0, has_side_effects=True, vmem_limit_bytes=60 * 1024 * 1024),
        )(dosage.reshape(groups, 8, slice_width))
        out = pl.pallas_call(
            functools.partial(finish_kernel, float(fields), share, vectors),
            out_shape=jax.ShapeDtypeStruct((share * 2 * vectors * 2, 4 * vectors), jnp.float32),
        )(total)
        return out.reshape(1, share, 2, vectors, 2, 4 * vectors)

    return jax.shard_map(
        body,
        mesh=mesh,
        in_specs=(P("vec", "field"),),
        out_specs=P("rep", ("vec", "field"), None, None, None, None),
        check_vma=False,
    )
```
